32 devices in a mesh: kv: 16 (over z, y, x), head: 2 (over core).
Axes of the slice: x: 2, y: 2, z: 4, core: 2. Of those that a mesh axis runs over, the one named last changes fastest.
Arguments:
- queries: bfloat16 [8, 256, 128], P('head', 'kv'), may hold values from -384 to 384
- key_cache: bfloat16 [4096, 8, 128, 128], P('kv', 'head'), may hold values from -6 to 6
- value_cache: bfloat16 [4096, 8, 128, 128], P('kv', 'head'), may hold values from -6 to 6
- key_new: bfloat16 [32, 8, 128], P(None, 'head'), may hold values from -6 to 6
- value_new: bfloat16 [32, 8, 128], P(None, 'head'), may hold values from -6 to 6
- lengths: int32 [32], replicated, may hold values from 2 to 16385, as said below
- page_table: int32 [4096], replicated, may hold values from 0 to 4095, each once
Outputs:
- attended: bfloat16 [8, 256, 128], P('head', 'kv')
The draws below stay inside these ranges and needn't reach their ends.
Inputs may be any that keep to these rules, and one draw needn't show every extreme that they name: The cache holds the first lengths[s] - 1 tokens of sequence s; some sequence has the largest length. `page_table`: every page appears once; page g lies on kv index g // 256.
All inputs are finite; a program needn't handle non-finite values.
Results may differ from the reference program's by a relative error of at most 0.0025.
Values may be sent and summed in bfloat16 or wider, within the bound.
A program may use at most 128 MiB of HBM per device.

```python
import math
import jax
import jax.numpy as jnp
from jax import lax

QH = 64
KVH = 8
HD = 128
PAGE = 128
MAXP = 128
SEQS = 32
PAGES = 4096


def draw_queries(key, part):
    normal_part = jax.random.normal(jax.random.fold_in(key, 11), (KVH, SEQS * (QH // KVH), HD), jnp.float32)
    values = jnp.clip(normal_part * 2.0, -8.0, 8.0)
    return values.astype(jnp.bfloat16)


def draw_lengths(key, part):
    most = MAXP * PAGE + 1
    values = jax.random.randint(jax.random.fold_in(key, 21), (SEQS,), 2, most + 1, jnp.int32)
    chosen = jax.random.randint(jax.random.fold_in(key, 22), (), 0, SEQS, jnp.int32)
    return jnp.where(jnp.arange(SEQS, dtype=jnp.int32) == chosen, most, values).astype(jnp.int32)


def block_levels(rng, shape, shards, low, largest):
    level, own = 1.0, jax.random.fold_in(rng, 6)
    for axis_at, shards_of in shards:
        draws = jnp.exp(jax.random.uniform(jax.random.fold_in(own, axis_at), (shards_of,), jnp.float32, low / len(shards), largest / len(shards)))
        level = level * jnp.repeat(draws, shape[axis_at] // shards_of).reshape([-1 if axis == axis_at else 1 for axis in range(len(shape))])
    return level


def noise(rng, dims, width, most, pieces=(), held_as=jnp.bfloat16):
    gain = block_levels(rng, dims, pieces, -0.22, 0.18) if pieces else 1.0
    entries = jax.random.normal(rng, dims, jnp.float32) * width * gain
    return jnp.minimum(jnp.maximum(entries, -most), most).astype(held_as)


def setup_inputs(seed: int = 0) -> dict:
    key_of = jax.random.split(jax.random.key(seed), 8)
    queries = draw_queries(jax.random.fold_in(key_of[7], 71), 0)
    key_cache = noise(key_of[1], (PAGES, KVH, PAGE, HD), 1.0, 6.0, ((0, 16), (1, 2)))
    value_cache = noise(key_of[2], (PAGES, KVH, PAGE, HD), 1.0, 6.0, ((0, 16), (1, 2)))
    key_new = noise(key_of[3], (SEQS, KVH, HD), 1.0, 6.0, ((1, 2),))
    value_new = noise(key_of[4], (SEQS, KVH, HD), 1.0, 6.0, ((1, 2),))
    lengths = draw_lengths(jax.random.fold_in(key_of[7], 71), 0)
    page_table = jax.random.permutation(key_of[6], PAGES).astype(jnp.int32)
    return {"queries": queries, "key_cache": key_cache, "value_cache": value_cache, "key_new": key_new, "value_new": value_new, "lengths": lengths, "page_table": page_table}


LOWEST_SCORE = -1e+30

def finish(cache_max, cache_sum, cache_out, query_wide, fresh_key, fresh_value, score_scale):
    new_score = lax.optimization_barrier(jnp.sum(query_wide * fresh_key.astype(jnp.float32), axis=-1)) * score_scale
    highest = jnp.maximum(cache_max, new_score)
    old_part = jnp.exp(cache_max - highest)
    new_part = jnp.exp(new_score - highest)
    numerator = cache_out * old_part[..., None] + new_part[..., None] * fresh_value.astype(jnp.float32)
    denominator = cache_sum * old_part + new_part
    return (numerator / denominator[..., None]).astype(jnp.bfloat16)

def reference(queries, key_cache, value_cache, key_new, value_new, lengths, page_table):
    seq_count = lengths.shape[0]
    kv_count = queries.shape[0]
    head_width = queries.shape[2]
    group_size = queries.shape[1] // seq_count
    page_total = key_cache.shape[0]
    page_len = key_cache.shape[2]
    page_slots = page_total // seq_count
    score_scale = 1.0 / math.sqrt(head_width)
    table = page_table.reshape(seq_count, page_slots).astype(jnp.int32)
    grouped = jnp.transpose(queries.reshape(kv_count, seq_count, group_size, head_width), (1, 0, 2, 3))
    offsets = jnp.arange(page_slots, dtype=jnp.int32)[:, None] * page_len + jnp.arange(page_len, dtype=jnp.int32)[None, :]

    def one_sequence(packed):
        query_rows, page_ids, length, fresh_key, fresh_value = packed
        keys = key_cache[page_ids].astype(jnp.float32)
        values = value_cache[page_ids].astype(jnp.float32)
        query_wide = query_rows.astype(jnp.float32)
        scores = jnp.einsum('gqd,mgtd->mgqt', query_wide, keys, precision=lax.Precision.HIGHEST) * score_scale
        in_cache = (offsets < length - 1)[:, None, None, :]
        masked = jnp.where(in_cache, scores, LOWEST_SCORE)
        page_max = lax.optimization_barrier(jnp.max(masked, axis=3))
        weights = jnp.where(in_cache, jnp.exp(masked - page_max[..., None]), 0.0)
        page_sum = lax.optimization_barrier(jnp.sum(weights, axis=3))
        rounded = lax.optimization_barrier(weights.astype(jnp.bfloat16)).astype(jnp.float32)
        page_out = jnp.einsum('mgqt,mgtd->mgqd', rounded, values, precision=lax.Precision.HIGHEST)
        cache_max = lax.optimization_barrier(jnp.max(page_max, axis=0))
        factor = jnp.exp(page_max - cache_max[None])
        cache_sum = lax.optimization_barrier(jnp.sum(page_sum * factor, axis=0))
        cache_out = lax.optimization_barrier(jnp.sum(page_out * factor[..., None], axis=0))
        return finish(cache_max, cache_sum, cache_out, query_wide, fresh_key[:, None, :], fresh_value[:, None, :], score_scale)
    result = lax.map(one_sequence, (grouped, table, lengths.astype(jnp.int32), key_new, value_new))
    return jnp.transpose(result, (1, 0, 2, 3)).reshape(kv_count, seq_count * group_size, head_width)
```

```python
import functools
import math

import jax
import jax.numpy as jnp
from jax import lax
from jax.experimental import pallas as pl
from jax.experimental.pallas import tpu as pltpu
from jax.sharding import PartitionSpec as P

LOWEST_SCORE = -1e30
MESH = pl.DeviceIdType.MESH
VMEM = pltpu.VMEM

GROUP = 16
RING = 4
LAG = 8
CHUNKS = 4
CODE = 32767.0
TINY = 1e-30

_dot = functools.partial(lax.dot_general, preferred_element_type=jnp.float32)
NT = (((1,), (1,)), ((), ()))
NN = (((1,), (0,)), ((), ()))


def greet(peers):
    barrier = pltpu.get_barrier_semaphore()
    for peer in peers:
        pl.semaphore_signal(barrier, inc=1, device_id={"kv": peer}, device_id_type=MESH)
    return lambda: pl.semaphore_wait(barrier, len(peers))


def split(n):
    plane = min(p for p in range(1, n + 1) if n % p == 0 and p * p >= n)
    return plane, n // plane


def nearest(line, lines):
    if lines & (lines - 1):
        return [lax.rem(line + k, lines) for k in range(1, lines)]
    others = []
    for k in range(1, lines):
        other, bit = line, 1
        while bit < lines:
            if k & bit:
                other = other + bit - 2 * bit * lax.rem(line // bit, 2)
            bit *= 2
        others.append(other)
    return others


def gather_kernel(
    n,
    pages_here,
    page_len,
    fetched,
    spare,
    x_ref,
    table_ref,
    length_ref,
    keys,
    values,
    all_ref,
    list_ref,
    key_ref,
    value_ref,
    table,
    length,
    send_sem,
    recv_sem,
    small_sem,
    page_sem,
):
    me = lax.axis_index("kv")
    plane, lines = split(n)
    spot, line = lax.rem(me, plane), me // plane
    beside = [line * plane + lax.rem(spot + k, plane) for k in range(1, plane)]
    floors = nearest(line, lines)
    arrived = greet(beside + [floor * plane + spot for floor in floors])
    small = [
        pltpu.make_async_copy(x_ref, all_ref.at[me], small_sem.at[0]),
        pltpu.make_async_copy(table_ref, table, small_sem.at[1]),
        pltpu.make_async_copy(length_ref, length, small_sem.at[2]),
    ]
    for copy in small:
        copy.start()
    bulk = []
    for c in range(CHUNKS):
        part = pl.ds(c * (fetched // CHUNKS), fetched // CHUNKS)
        bulk.append(pltpu.make_async_copy(keys.at[part], key_ref.at[part], page_sem.at[0, c]))
        bulk.append(pltpu.make_async_copy(values.at[part], value_ref.at[part], page_sem.at[1, c]))
    for copy in bulk:
        copy.start()
    for copy in small:
        copy.wait()

    def block(source, k, target):
        return pltpu.make_async_remote_copy(
            src_ref=all_ref.at[source],
            dst_ref=all_ref.at[source],
            send_sem=send_sem.at[k],
            recv_sem=recv_sem.at[source],
            device_id={"kv": target},
            device_id_type=MESH,
        )

    state = rank_pages(me, pages_here, page_len, fetched, spare, table, length)
    arrived()
    copies = []

    def send(source, target):
        copy = block(source, len(copies), target)
        copy.start()
        copies.append(copy)

    for floor in floors[::-1]:
        send(me, floor * plane + spot)
    for other in beside:
        send(me, other)
    list_pages(state, list_ref)
    for floor in floors:
        source = floor * plane + spot
        block(source, 0, source).wait_recv()
        for other in beside:
            send(source, other)
    for floor in [line] + floors:
        for k in range(1, plane):
            source = floor * plane + lax.rem(spot + k, plane)
            block(source, 0, source).wait_recv()
    for copy in copies:
        copy.wait_send()
    for copy in bulk:
        copy.wait()


def rank_pages(me, pages_here, page_len, fetched, spare, table_ref, length_ref):
    seqs, slots = table_ref.shape
    page = table_ref[...] - me * pages_here
    line = lax.broadcasted_iota(jnp.int32, (seqs, slots), 0)
    length = jnp.zeros((seqs, slots), jnp.int32)
    for s in range(seqs):
        length = jnp.where(line == s, length_ref[s], length)
    tokens = length - 1 - lax.broadcasted_iota(jnp.int32, (seqs, slots), 1) * page_len
    wanted = (page >= 0) & (page < pages_here) & (tokens > 0)
    ready = wanted & (page < fetched)
    early = jnp.where(ready, 1.0, 0.0)
    late = jnp.where(wanted, 1.0, 0.0) - early
    upto = jnp.where(
        lax.broadcasted_iota(jnp.int32, (slots, slots), 0)
        <= lax.broadcasted_iota(jnp.int32, (slots, slots), 1),
        1.0,
        0.0,
    ).astype(jnp.bfloat16)
    before = jnp.where(
        lax.broadcasted_iota(jnp.int32, (seqs, seqs), 1)
        < lax.broadcasted_iota(jnp.int32, (seqs, seqs), 0),
        1.0,
        0.0,
    ).astype(jnp.bfloat16)

    def place(flag):
        inside = _dot(flag.astype(jnp.bfloat16), upto, NN)
        total = jnp.broadcast_to(jnp.sum(flag, axis=1, keepdims=True), (seqs, slots))
        offset = _dot(before, total.astype(jnp.bfloat16), NN)
        count = jnp.sum(jnp.sum(flag, axis=1, keepdims=True), axis=0, keepdims=True)
        return inside + offset - 1.0, count

    early_rank, early_count = place(early)
    late_rank, late_count = place(late)
    rank = jnp.where(
        ready, early_rank, jnp.where(wanted, late_rank + early_count, -1.0)
    ).astype(jnp.int32)
    ring = fetched + lax.rem(jnp.where(wanted, late_rank, 0.0).astype(jnp.int32), spare)
    wide = jnp.where(wanted, page, 0).astype(jnp.float32)
    slot = jnp.where(ready, page, jnp.where(wanted, ring, 0)).astype(jnp.float32)
    held = jnp.where(wanted, jnp.minimum(tokens, page_len), 0).astype(jnp.float32)
    return rank, wide, slot, held, early_count, early_count + late_count


def list_pages(state, list_ref):
    rank, wide, slot, held, early_count, count = state
    seqs, slots = rank.shape
    listed = list_ref.shape[1]
    row = lax.broadcasted_iota(jnp.int32, (8, slots), 0)
    place = lax.broadcasted_iota(jnp.int32, (listed, slots), 0)
    out = jnp.zeros((8, listed), jnp.float32)
    for s in range(seqs):

        def rows(x):
            return jnp.broadcast_to(x[s : s + 1], (8, slots))

        values = jnp.where(
            row == 0,
            float(s),
            jnp.where(
                row == 1,
                rows(slot),
                jnp.where(row == 2, rows(wide), jnp.where(row == 3, rows(held), 0.0)),
            ),
        ).astype(jnp.bfloat16)
        chosen = jnp.where(
            place == jnp.broadcast_to(rank[s : s + 1], (listed, slots)), 1.0, 0.0
        ).astype(jnp.bfloat16)
        out = out + _dot(values, chosen, NT)
    line = lax.broadcasted_iota(jnp.int32, (8, listed), 0)
    out = jnp.where(line == 4, jnp.broadcast_to(count, (8, listed)), out)
    out = jnp.where(line == 5, jnp.broadcast_to(early_count, (8, listed)), out)
    list_ref[...] = out.astype(jnp.int32)


def attend_kernel(
    group_rows,
    blocks,
    lines,
    list_ref,
    q_ref,
    keys,
    values,
    key_in,
    value_in,
    code_ref,
    stat_ref,
    key_buf,
    value_buf,
    q_wide,
    score,
    best,
    weight,
    total,
    key_sem,
    value_sem,
):
    heads, page_len, width = key_buf.shape[1:]
    seqs = q_wide.shape[0]
    per_block = seqs // blocks
    scale2 = math.log2(math.e) / math.sqrt(width)
    count = list_ref[4, 0]
    early = list_ref[5, 0]
    groups = (count + GROUP - 1) // GROUP
    ready = early // GROUP

    def copies(g, i):
        at = g * GROUP + i
        page, slot, ring = list_ref[2, at], list_ref[1, at], lax.rem(g, RING)
        return (
            pltpu.make_async_copy(keys.at[page], key_buf.at[slot], key_sem.at[ring]),
            pltpu.make_async_copy(values.at[page], value_buf.at[slot], value_sem.at[ring]),
        )

    def whole(g):
        return (g * GROUP >= early) & ((g + 1) * GROUP <= count)

    def mixed(g):
        return jnp.logical_not(whole(g)) & ((g + 1) * GROUP > early)

    def each(g, act):
        def item(i, carry):
            at = g * GROUP + i

            @pl.when((at >= early) & (at < count))
            def _():
                for copy in copies(g, i):
                    act(copy)

            return carry

        lax.fori_loop(0, GROUP, item, 0)

    def start(g):
        @pl.when(whole(g))
        def _():
            for i in range(GROUP):
                for copy in copies(g, i):
                    copy.start()

        @pl.when(mixed(g))
        def _():
            each(g, lambda copy: copy.start())

    def wait(g):
        @pl.when(whole(g))
        def _():
            ring, part = lax.rem(g, RING), pl.ds(0, GROUP)
            pltpu.make_async_copy(keys.at[part], key_buf.at[part], key_sem.at[ring]).wait()
            pltpu.make_async_copy(values.at[part], value_buf.at[part], value_sem.at[ring]).wait()

        @pl.when(mixed(g))
        def _():
            each(g, lambda copy: copy.wait())

    def first(g, carry):
        start(g)
        return carry

    lax.fori_loop(ready, jnp.minimum(groups, ready + RING), first, 0)

    best[...] = jnp.full(best.shape, LOWEST_SCORE, jnp.float32)
    weight[...] = jnp.zeros(weight.shape, jnp.float32)
    total[...] = jnp.zeros(total.shape, jnp.float32)
    rows = q_ref.shape[2]
    for s in range(seqs):
        for pair in range(heads // 2):
            lines_of = []
            for h in (2 * pair, 2 * pair + 1):
                if rows >= group_rows:
                    per = rows // group_rows
                    d, j = s // per, s % per
                    wide = q_ref[d, h].astype(jnp.float32)
                    lines_of.append(wide[j * group_rows : (j + 1) * group_rows])
                else:
                    per = group_rows // rows
                    lines_of += [q_ref[s * per + e, h].astype(jnp.float32) for e in range(per)]
            q_wide[s, pair] = jnp.concatenate(lines_of, axis=0).astype(q_wide.dtype)

    lane = lax.broadcasted_iota(jnp.int32, (group_rows, page_len), 1)
    both = [(i, pair) for i in range(GROUP) for pair in range(heads // 2)]
    every = [(i, h) for i in range(GROUP) for h in range(heads)]

    def ask(g, i, pair):
        seq, slot = list_ref[0, g * GROUP + i], list_ref[1, g * GROUP + i]
        k2 = key_buf[slot, 2 * pair : 2 * pair + 2].reshape(2 * page_len, width)
        found = _dot(q_wide[seq, pair], k2, NT)
        for e in range(2):
            score[i, 2 * pair + e] = found[
                e * group_rows : (e + 1) * group_rows, e * page_len : (e + 1) * page_len
            ]

    def soften(g):
        lengths = [list_ref[3, g * GROUP + i] for i in range(GROUP)]
        scores, tops, weights, keeps, adds = {}, {}, {}, {}, {}
        for i, h in every:
            sc = jnp.where(lane < lengths[i], score[i, h], LOWEST_SCORE)
            scores[i, h] = sc
            tops[i, h] = jnp.broadcast_to(jnp.max(sc, axis=1, keepdims=True), sc.shape)
        for i, h in every:
            seq = list_ref[0, g * GROUP + i]
            found = jnp.where(
                lane < lengths[i], jnp.exp2((scores[i, h] - tops[i, h]) * scale2), 0.0
            )
            old = best[seq, h]
            new = jnp.maximum(old, tops[i, h])
            best[seq, h] = new
            keeps[i, h] = jnp.exp2((old - new) * scale2)
            adds[i, h] = jnp.exp2((tops[i, h] - new) * scale2)
            weight[seq, h] = weight[seq, h] * keeps[i, h] + found * adds[i, h]
            weights[i, h] = found
        return weights, keeps, adds

    def take(g, i, pair, softened):
        weights, keeps, adds = softened
        seq, slot = list_ref[0, g * GROUP + i], list_ref[1, g * GROUP + i]
        w2 = jnp.concatenate([weights[i, 2 * pair], weights[i, 2 * pair + 1]], axis=0)
        v2 = jnp.concatenate([value_buf[slot, 2 * pair], value_buf[slot, 2 * pair + 1]], axis=1)
        found = _dot(w2.astype(jnp.bfloat16), v2, NN)
        for e in range(2):
            h = 2 * pair + e
            mine = found[e * group_rows : (e + 1) * group_rows, e * width : (e + 1) * width]
            total[seq, h] = total[seq, h] * keeps[i, h] + mine * adds[i, h]

    wait(0)
    for i, pair in both:
        ask(0, i, pair)

    def step(g, carry):
        pl.when((g >= ready + 2) & (g + RING - 2 < groups))(lambda: start(g + RING - 2))
        wait(g)
        softened = soften(g - 1)
        for at in range(len(both) + LAG):
            if at >= LAG:
                take(g - 1, *both[at - LAG], softened)
            if at < len(both):
                ask(g, *both[at])
        return carry

    lax.fori_loop(1, groups, step, 0)
    last = jnp.maximum(groups - 1, 0)
    softened = soften(last)
    for i, pair in both:
        take(last, i, pair, softened)

    columns = heads * per_block
    across = blocks // lines
    fit = 128 // (3 * columns)
    stat_lane = lax.broadcasted_iota(jnp.int32, (group_rows, width), 1)
    for a in range(across):
        stats = {}
        for floor in range(lines):
            b = floor * across + a
            tile, base = floor // fit, (floor % fit) * 3 * columns
            stat = stats.get(tile, jnp.zeros((group_rows, width), jnp.float32))
            coded = []
            for c in range(columns):
                h, s = c // per_block, b * per_block + c % per_block
                sums = total[s, h]
                mass = jnp.sum(weight[s, h], axis=1, keepdims=True)
                largest = jnp.maximum(jnp.max(jnp.abs(sums), axis=1, keepdims=True), TINY)
                coded.append(jnp.round(sums * (CODE / largest)))
                stat = jnp.where(stat_lane == base + c, best[s, h], stat)
                stat = jnp.where(
                    stat_lane == base + columns + c, jnp.broadcast_to(mass, stat.shape), stat
                )
                stat = jnp.where(
                    stat_lane == base + 2 * columns + c,
                    jnp.broadcast_to(largest * (1.0 / CODE), stat.shape),
                    stat,
                )
            stats[tile] = stat
            for c in range(0, columns, 2):
                code_ref[b, c * group_rows : (c + 2) * group_rows] = (
                    jnp.concatenate(coded[c : c + 2], axis=0)
                    .astype(jnp.int32)
                    .astype(code_ref.dtype)
                )
        for tile, stat in stats.items():
            stat_ref[a, tile] = stat


def fold(codes, stats, columns, group_rows, scale2):
    top = functools.reduce(jnp.maximum, stats)
    lanes = top.shape[1]
    mass = jnp.zeros_like(top)
    sizes = []
    for stat in stats:
        factor = jnp.exp2((stat - top) * scale2)
        mass = mass + stat * pltpu.roll(factor, columns, 1)
        sizes.append(factor * pltpu.roll(stat, lanes - 2 * columns, 1))
    return top, mass, sizes


def combine(codes, sizes, columns, group_rows):
    sums = [jnp.zeros_like(sizes[0]) for _ in range(columns)]
    for code, size in zip(codes, sizes):
        wide = code[...].astype(jnp.int32).astype(jnp.float32)
        for c in range(columns):
            sums[c] = sums[c] + wide[c * group_rows : (c + 1) * group_rows] * jnp.broadcast_to(
                size[:, c : c + 1], size.shape
            )
    return sums


def exchange_kernel(
    n,
    parts,
    heads,
    code_ref,
    stat_ref,
    q_ref,
    key_ref,
    value_ref,
    out_ref,
    near,
    near_stat,
    folded,
    folded_stat,
    far,
    far_stat,
    near_send,
    near_recv,
    stat_send,
    stat_recv,
    far_send,
    far_recv,
):
    me = lax.axis_index("kv")
    plane, lines = split(n)
    spot, line = lax.rem(me, plane), me // plane
    group_rows, width = stat_ref.shape[2:]
    columns = code_ref.shape[1] // group_rows
    per_block = columns // heads
    across = plane // parts
    fit = 128 // (3 * columns)
    scale2 = math.log2(math.e) / math.sqrt(width)
    spots = [lax.rem(spot + k, plane) for k in range(1, plane)]
    floors = nearest(line, lines)[::-1] + [line]
    arrived = greet([line * plane + p for p in spots] + [f * plane + spot for f in floors[:-1]])

    def stat_copy(p, other, source):
        return pltpu.make_async_remote_copy(
            src_ref=stat_ref.at[other // parts],
            dst_ref=near_stat.at[source],
            send_sem=stat_send.at[p],
            recv_sem=stat_recv.at[source],
            device_id={"kv": line * plane + other},
            device_id_type=MESH,
        )

    def near_copy(k, floor, p, other, source):
        return pltpu.make_async_remote_copy(
            src_ref=code_ref.at[floor * across + other // parts],
            dst_ref=near.at[floor, source],
            send_sem=near_send.at[k, p],
            recv_sem=near_recv.at[floor, source],
            device_id={"kv": line * plane + other},
            device_id_type=MESH,
        )

    def far_copies(k, floor, source):
        return [
            pltpu.make_async_remote_copy(
                src_ref=src.at[k],
                dst_ref=dst.at[source],
                send_sem=far_send.at[e, k],
                recv_sem=far_recv.at[e, source],
                device_id={"kv": floor * plane + spot},
                device_id_type=MESH,
            )
            for e, (src, dst) in enumerate(((folded_stat, far_stat), (folded, far)))
        ]

    arrived()
    copies = []

    def send(copy):
        copy.start()
        copies.append(copy)

    for p, other in enumerate(spots):
        send(stat_copy(p, other, spot))
    for k, floor in enumerate(floors):
        for p, other in enumerate(spots):
            send(near_copy(k, floor, p, other, spot))
    for p, other in enumerate(spots):
        stat_copy(p, other, other).wait_recv()

    def aligned(ref, index, floor):
        if fit >= lines:
            tile, at = ref[index, 0], floor
        else:
            tile, at = ref[index, floor // fit], lax.rem(floor, fit)
        return pltpu.roll(tile, lax.rem(width - at * 3 * columns, width), 1)

    stat_lane = lax.broadcasted_iota(jnp.int32, (group_rows, width), 1)
    own = None
    for k, floor in enumerate(floors):
        stats = [aligned(stat_ref, spot // parts, floor)]
        stats += [aligned(near_stat, other, floor) for other in spots]
        for p, other in enumerate(spots):
            near_copy(k, floor, p, other, other).wait_recv()
        codes = [code_ref.at[floor * across + spot // parts]]
        codes += [near.at[floor, other] for other in spots]
        top, mass, sizes = fold(codes, stats, columns, group_rows, scale2)
        if k == lines - 1:
            own = top, mass, combine(codes, sizes, columns, group_rows)
            break
        size = jnp.maximum(functools.reduce(jnp.add, sizes), TINY)
        inverse = 1.0 / size
        sums = combine(codes, [s * inverse for s in sizes], columns, group_rows)
        folded_stat[k] = jnp.where(
            stat_lane < columns,
            top,
            jnp.where(stat_lane < 2 * columns, mass, pltpu.roll(size, 2 * columns, 1)),
        )
        for c in range(0, columns, 2):
            folded[k, c * group_rows : (c + 2) * group_rows] = (
                jnp.round(jnp.concatenate(sums[c : c + 2], axis=0))
                .astype(jnp.int32)
                .astype(folded.dtype)
            )
        for copy in far_copies(k, floor, line):
            send(copy)
    for k, floor in enumerate(floors[:-1]):
        for copy in far_copies(k, floor, floor):
            copy.wait_recv()
    stats = [far_stat[floor] for floor in floors[:-1]]
    own_top, own_mass, own_sums = own
    top = functools.reduce(jnp.maximum, stats, own_top)
    own_factor = jnp.exp2((own_top - top) * scale2)
    mass = own_mass * pltpu.roll(own_factor, columns, 1)
    sums = [s * jnp.broadcast_to(own_factor[:, c : c + 1], s.shape) for c, s in enumerate(own_sums)]
    sizes = []
    for stat in stats:
        factor = jnp.exp2((stat - top) * scale2)
        mass = mass + stat * pltpu.roll(factor, columns, 1)
        sizes.append(factor * pltpu.roll(stat, width - 2 * columns, 1))
    more = combine([far.at[floor] for floor in floors[:-1]], sizes, columns, group_rows)
    sums = [a + b for a, b in zip(sums, more)]
    for h in range(heads):
        wide = q_ref[h].astype(jnp.float32)
        results = []
        for j in range(per_block):
            c = h * per_block + j
            s = (me // parts) * per_block + j
            rows = slice(j * group_rows, (j + 1) * group_rows) if parts == 1 else slice(None)
            query = wide[rows]
            shape = query.shape
            fresh_key = jnp.broadcast_to(key_ref[s][h : h + 1].astype(jnp.float32), shape)
            fresh_value = jnp.broadcast_to(value_ref[s][h : h + 1].astype(jnp.float32), shape)
            new = jnp.broadcast_to(jnp.sum(query * fresh_key, axis=1, keepdims=True), shape)

            def mine(x):
                if parts == 1:
                    return x
                size = group_rows // parts
                picked = x[:size]
                for p in range(1, parts):
                    picked = jnp.where(
                        lax.rem(me, parts) == p, x[p * size : (p + 1) * size], picked
                    )
                return picked

            old = mine(jnp.broadcast_to(top[:, c : c + 1], top.shape))
            old_mass = mine(jnp.broadcast_to(mass[:, columns + c : columns + c + 1], top.shape))
            old_sum = mine(sums[c])
            highest = jnp.maximum(old, new)
            old_part = jnp.exp2((old - highest) * scale2)
            new_part = jnp.exp2((new - highest) * scale2)
            results.append(
                (old_sum * old_part + new_part * fresh_value) / (old_mass * old_part + new_part)
            )
        out_ref[h] = jnp.concatenate(results, axis=0).astype(out_ref.dtype)
    for copy in copies:
        copy.wait_send()


def far_off(x):
    return pltpu.with_memory_space_constraint(x, pltpu.HBM)


def on_device(n, queries, key_cache, value_cache, key_new, value_new, lengths, page_table):
    heads, local_rows, width = queries.shape
    seqs = lengths.shape[0]
    slots = page_table.shape[0] // seqs
    pages_here, _, page_len, _ = key_cache.shape
    group_rows = local_rows * n // seqs
    parts = max(1, group_rows // local_rows)
    blocks = n // parts
    columns = heads * (seqs // blocks)
    plane, lines = split(n)
    listed = -(-(pages_here + GROUP) // 128) * 128
    fetched = pages_here // 4
    spare = GROUP * RING
    held = fetched + spare
    tiles = -(-lines // (128 // (3 * columns)))
    vmem = pl.BlockSpec(memory_space=VMEM)
    smem = pl.BlockSpec(memory_space=pltpu.SMEM)
    hbm = pl.BlockSpec(memory_space=pltpu.HBM)
    sends = (lines - 1) + (plane - 1) * lines

    every_query, pages, key_buf, value_buf = pl.pallas_call(
        functools.partial(gather_kernel, n, pages_here, page_len, fetched, spare),
        out_shape=(
            jax.ShapeDtypeStruct((n,) + queries.shape, queries.dtype),
            jax.ShapeDtypeStruct((8, listed), jnp.int32),
            VMEM((held,) + key_cache.shape[1:], key_cache.dtype),
            VMEM((held,) + value_cache.shape[1:], value_cache.dtype),
        ),
        in_specs=[hbm] * 5,
        out_specs=(vmem, vmem, vmem, vmem),
        scratch_shapes=[
            VMEM((seqs, slots), jnp.int32),
            pltpu.SMEM((seqs,), jnp.int32),
            pltpu.SemaphoreType.DMA((sends,)),
            pltpu.SemaphoreType.DMA((n,)),
            pltpu.SemaphoreType.DMA((3,)),
            pltpu.SemaphoreType.DMA((2, CHUNKS)),
        ],
        compiler_params=pltpu.CompilerParams(
            collective_id=0, has_side_effects=True, vmem_limit_bytes=6 * 1024 * 1024
        ),
        name="gather_queries",
    )(far_off(queries), far_off(page_table.reshape(seqs, slots)), far_off(lengths), key_cache, value_cache)

    codes, stats, _, _ = pl.pallas_call(
        functools.partial(attend_kernel, group_rows, blocks, lines),
        out_shape=(
            jax.ShapeDtypeStruct((blocks, columns * group_rows, width), jnp.int16),
            jax.ShapeDtypeStruct((plane // parts, tiles, group_rows, width), jnp.float32),
            VMEM(key_buf.shape, key_buf.dtype),
            VMEM(value_buf.shape, value_buf.dtype),
        ),
        in_specs=[smem, vmem, hbm, hbm, vmem, vmem],
        out_specs=(vmem, vmem, vmem, vmem),
        input_output_aliases={4: 2, 5: 3},
        scratch_shapes=[
            VMEM((seqs, heads // 2, 2 * group_rows, width), queries.dtype),
            VMEM((GROUP, heads, group_rows, page_len), jnp.float32),
            VMEM((seqs, heads, group_rows, page_len), jnp.float32),
            VMEM((seqs, heads, group_rows, page_len), jnp.float32),
            VMEM((seqs, heads, group_rows, width), jnp.float32),
            pltpu.SemaphoreType.DMA((RING,)),
            pltpu.SemaphoreType.DMA((RING,)),
        ],
        compiler_params=pltpu.CompilerParams(vmem_limit_bytes=10 * 1024 * 1024),
        name="attend_pages",
    )(pages, every_query, key_cache, value_cache, key_buf, value_buf)

    code = (columns * group_rows, width)
    stat = (group_rows, width)
    return pl.pallas_call(
        functools.partial(exchange_kernel, n, parts, heads),
        out_shape=jax.ShapeDtypeStruct(queries.shape, jnp.bfloat16),
        in_specs=[vmem] * 5,
        out_specs=vmem,
        scratch_shapes=[
            VMEM((lines, plane) + code, jnp.int16),
            VMEM((plane, tiles) + stat, jnp.float32),
            VMEM((lines,) + code, jnp.int16),
            VMEM((lines,) + stat, jnp.float32),
            VMEM((lines,) + code, jnp.int16),
            VMEM((lines,) + stat, jnp.float32),
            pltpu.SemaphoreType.DMA((lines, plane)),
            pltpu.SemaphoreType.DMA((lines, plane)),
            pltpu.SemaphoreType.DMA((plane,)),
            pltpu.SemaphoreType.DMA((plane,)),
            pltpu.SemaphoreType.DMA((2, lines)),
            pltpu.SemaphoreType.DMA((2, lines)),
        ],
        compiler_params=pltpu.CompilerParams(
            collective_id=1, has_side_effects=True, vmem_limit_bytes=16 * 1024 * 1024
        ),
        name="exchange_and_finish",
    )(codes, stats, queries, key_new, value_new)


def solution(mesh):
    placed = (
        P("head", "kv", None),
        P("kv", "head", None, None),
        P("kv", "head", None, None),
        P(None, "head", None),
        P(None, "head", None),
        P(),
        P(),
    )
    return jax.shard_map(
        functools.partial(on_device, mesh.shape["kv"]),
        mesh=mesh,
        in_specs=placed,
        out_specs=P("head", "kv", None),
        check_vma=False,
    )
```

```python
import functools
import math

import jax
import jax.numpy as jnp
from jax import lax
from jax.experimental import pallas as pl
from jax.experimental.pallas import tpu as pltpu
from jax.sharding import PartitionSpec as P

LOWEST_SCORE = -1e30
MESH = pl.DeviceIdType.MESH
VMEM = pltpu.VMEM

GROUP = 8
RING = 8
LAG = 8
CHUNKS = 4
CODE = 32767.0
TINY = 1e-30

_dot = functools.partial(lax.dot_general, preferred_element_type=jnp.float32)
NT = (((1,), (1,)), ((), ()))
NN = (((1,), (0,)), ((), ()))


def greet(peers):
    barrier = pltpu.get_barrier_semaphore()
    for peer in peers:
        pl.semaphore_signal(barrier, inc=1, device_id={"kv": peer}, device_id_type=MESH)
    return lambda: pl.semaphore_wait(barrier, len(peers))


def split(n):
    plane = min(p for p in range(1, n + 1) if n % p == 0 and p * p >= n)
    return plane, n // plane


def nearest(line, lines):
    if lines & (lines - 1):
        return [lax.rem(line + k, lines) for k in range(1, lines)]
    others = []
    for k in range(1, lines):
        other, bit = line, 1
        while bit < lines:
            if k & bit:
                other = other + bit - 2 * bit * lax.rem(line // bit, 2)
            bit *= 2
        others.append(other)
    return others


def gather_kernel(
    n,
    pages_here,
    page_len,
    fetched,
    spare,
    x_ref,
    table_ref,
    length_ref,
    keys,
    values,
    all_ref,
    list_ref,
    key_ref,
    value_ref,
    table,
    length,
    send_sem,
    recv_sem,
    small_sem,
    page_sem,
):
    me = lax.axis_index("kv")
    plane, lines = split(n)
    spot, line = lax.rem(me, plane), me // plane
    beside = [line * plane + lax.rem(spot + k, plane) for k in range(1, plane)]
    floors = nearest(line, lines)
    arrived = greet(beside + [floor * plane + spot for floor in floors])
    small = [
        pltpu.make_async_copy(x_ref, all_ref.at[me], small_sem.at[0]),
        pltpu.make_async_copy(table_ref, table, small_sem.at[1]),
        pltpu.make_async_copy(length_ref, length, small_sem.at[2]),
    ]
    for copy in small:
        copy.start()
    for copy in small:
        copy.wait()
    bulk = []
    for c in range(CHUNKS):
        part = pl.ds(c * (fetched // CHUNKS), fetched // CHUNKS)
        bulk.append(pltpu.make_async_copy(keys.at[part], key_ref.at[part], page_sem.at[0, c]))
        bulk.append(pltpu.make_async_copy(values.at[part], value_ref.at[part], page_sem.at[1, c]))
    for copy in bulk:
        copy.start()

    def block(source, k, target):
        return pltpu.make_async_remote_copy(
            src_ref=all_ref.at[source],
            dst_ref=all_ref.at[source],
            send_sem=send_sem.at[k],
            recv_sem=recv_sem.at[source],
            device_id={"kv": target},
            device_id_type=MESH,
        )

    arrived()
    copies = []

    def send(source, target):
        copy = block(source, len(copies), target)
        copy.start()
        copies.append(copy)

    for floor in floors[::-1]:
        send(me, floor * plane + spot)
    for other in beside:
        send(me, other)
    list_pages(rank_pages(me, pages_here, page_len, fetched, spare, table, length), list_ref)
    for floor in floors:
        source = floor * plane + spot
        block(source, 0, source).wait_recv()
        for other in beside:
            send(source, other)
    for floor in [line] + floors:
        for k in range(1, plane):
            source = floor * plane + lax.rem(spot + k, plane)
            block(source, 0, source).wait_recv()
    for copy in copies:
        copy.wait_send()
    for copy in bulk:
        copy.wait()


def rank_pages(me, pages_here, page_len, fetched, spare, table_ref, length_ref):
    seqs, slots = table_ref.shape
    page = table_ref[...] - me * pages_here
    line = lax.broadcasted_iota(jnp.int32, (seqs, slots), 0)
    length = jnp.zeros((seqs, slots), jnp.int32)
    for s in range(seqs):
        length = jnp.where(line == s, length_ref[s], length)
    tokens = length - 1 - lax.broadcasted_iota(jnp.int32, (seqs, slots), 1) * page_len
    wanted = (page >= 0) & (page < pages_here) & (tokens > 0)
    ready = wanted & (page < fetched)
    early = jnp.where(ready, 1.0, 0.0)
    late = jnp.where(wanted, 1.0, 0.0) - early
    upto = jnp.where(
        lax.broadcasted_iota(jnp.int32, (slots, slots), 0)
        <= lax.broadcasted_iota(jnp.int32, (slots, slots), 1),
        1.0,
        0.0,
    ).astype(jnp.bfloat16)
    before = jnp.where(
        lax.broadcasted_iota(jnp.int32, (seqs, seqs), 1)
        < lax.broadcasted_iota(jnp.int32, (seqs, seqs), 0),
        1.0,
        0.0,
    ).astype(jnp.bfloat16)

    def place(flag):
        inside = _dot(flag.astype(jnp.bfloat16), upto, NN)
        total = jnp.broadcast_to(jnp.sum(flag, axis=1, keepdims=True), (seqs, slots))
        offset = _dot(before, total.astype(jnp.bfloat16), NN)
        count = jnp.sum(jnp.sum(flag, axis=1, keepdims=True), axis=0, keepdims=True)
        return inside + offset - 1.0, count

    early_rank, early_count = place(early)
    late_rank, late_count = place(late)
    rank = jnp.where(
        ready, early_rank, jnp.where(wanted, late_rank + early_count, -1.0)
    ).astype(jnp.int32)
    ring = fetched + lax.rem(jnp.where(wanted, late_rank, 0.0).astype(jnp.int32), spare)
    wide = jnp.where(wanted, page, 0).astype(jnp.float32)
    slot = jnp.where(ready, page, jnp.where(wanted, ring, 0)).astype(jnp.float32)
    held = jnp.where(wanted, jnp.minimum(tokens, page_len), 0).astype(jnp.float32)
    return rank, wide, slot, held, early_count, early_count + late_count


def list_pages(state, list_ref):
    rank, wide, slot, held, early_count, count = state
    seqs, slots = rank.shape
    listed = list_ref.shape[1]
    row = lax.broadcasted_iota(jnp.int32, (8, slots), 0)
    place = lax.broadcasted_iota(jnp.int32, (listed, slots), 0)
    out = jnp.zeros((8, listed), jnp.float32)
    for s in range(seqs):

        def rows(x):
            return jnp.broadcast_to(x[s : s + 1], (8, slots))

        values = jnp.where(
            row == 0,
            float(s),
            jnp.where(
                row == 1,
                rows(slot),
                jnp.where(row == 2, rows(wide), jnp.where(row == 3, rows(held), 0.0)),
            ),
        ).astype(jnp.bfloat16)
        chosen = jnp.where(
            place == jnp.broadcast_to(rank[s : s + 1], (listed, slots)), 1.0, 0.0
        ).astype(jnp.bfloat16)
        out = out + _dot(values, chosen, NT)
    line = lax.broadcasted_iota(jnp.int32, (8, listed), 0)
    out = jnp.where(line == 4, jnp.broadcast_to(count, (8, listed)), out)
    out = jnp.where(line == 5, jnp.broadcast_to(early_count, (8, listed)), out)
    list_ref[...] = out.astype(jnp.int32)


def attend_kernel(
    group_rows,
    blocks,
    lines,
    list_ref,
    q_ref,
    keys,
    values,
    key_in,
    value_in,
    code_ref,
    stat_ref,
    key_buf,
    value_buf,
    q_wide,
    score,
    best,
    weight,
    total,
    key_sem,
    value_sem,
):
    heads, page_len, width = key_buf.shape[1:]
    seqs = q_wide.shape[0]
    per_block = seqs // blocks
    scale2 = math.log2(math.e) / math.sqrt(width)
    count = list_ref[4, 0]
    early = list_ref[5, 0]
    groups = (count + GROUP - 1) // GROUP
    late = count - early
    held_groups = (early + GROUP - 1) // GROUP
    full = late // GROUP
    rest = lax.rem(late, GROUP)

    def copies(q, i):
        at = early + q * GROUP + i
        page, slot, ring = list_ref[2, at], list_ref[1, at], lax.rem(q, RING)
        return (
            pltpu.make_async_copy(keys.at[page], key_buf.at[slot], key_sem.at[ring]),
            pltpu.make_async_copy(values.at[page], value_buf.at[slot], value_sem.at[ring]),
        )

    def issue(q, i):
        for copy in copies(q, i):
            copy.start()

    def some(q, act):
        def item(i, carry):
            for copy in copies(q, i):
                act(copy)
            return carry

        lax.fori_loop(0, rest, item, 0)

    def start_rest(q):
        pl.when((q == full) & (rest > 0))(lambda: some(q, lambda copy: copy.start()))

    def wait(q):
        @pl.when((q >= 0) & (q < full))
        def _():
            ring, part = lax.rem(q, RING), pl.ds(0, GROUP)
            pltpu.make_async_copy(keys.at[part], key_buf.at[part], key_sem.at[ring]).wait()
            pltpu.make_async_copy(values.at[part], value_buf.at[part], value_sem.at[ring]).wait()

        pl.when((q == full) & (rest > 0))(lambda: some(q, lambda copy: copy.wait()))

    def first(q, carry):
        for i in range(GROUP):
            issue(q, i)
        return carry

    lax.fori_loop(0, jnp.minimum(full, RING), first, 0)
    pl.when(full < RING)(lambda: start_rest(full))

    best[...] = jnp.full(best.shape, LOWEST_SCORE, jnp.float32)
    weight[...] = jnp.zeros(weight.shape, jnp.float32)
    total[...] = jnp.zeros(total.shape, jnp.float32)
    rows = q_ref.shape[2]
    for s in range(seqs):
        for pair in range(heads // 2):
            lines_of = []
            for h in (2 * pair, 2 * pair + 1):
                if rows >= group_rows:
                    per = rows // group_rows
                    d, j = s // per, s % per
                    wide = q_ref[d, h].astype(jnp.float32)
                    lines_of.append(wide[j * group_rows : (j + 1) * group_rows])
                else:
                    per = group_rows // rows
                    lines_of += [q_ref[s * per + e, h].astype(jnp.float32) for e in range(per)]
            q_wide[s, pair] = jnp.concatenate(lines_of, axis=0).astype(q_wide.dtype)

    lane = lax.broadcasted_iota(jnp.int32, (group_rows, page_len), 1)
    both = [(i, pair) for i in range(GROUP) for pair in range(heads // 2)]
    every = [(i, h) for i in range(GROUP) for h in range(heads)]

    def ask(g, i, pair):
        seq, slot = list_ref[0, g * GROUP + i], list_ref[1, g * GROUP + i]
        k2 = key_buf[slot, 2 * pair : 2 * pair + 2].reshape(2 * page_len, width)
        found = _dot(q_wide[seq, pair], k2, NT)
        for e in range(2):
            score[i, 2 * pair + e] = found[
                e * group_rows : (e + 1) * group_rows, e * page_len : (e + 1) * page_len
            ]

    def soften(g):
        lengths = [list_ref[3, g * GROUP + i] for i in range(GROUP)]
        scores, tops, weights, keeps, adds = {}, {}, {}, {}, {}
        for i, h in every:
            sc = jnp.where(lane < lengths[i], score[i, h], LOWEST_SCORE)
            scores[i, h] = sc
            tops[i, h] = jnp.broadcast_to(jnp.max(sc, axis=1, keepdims=True), sc.shape)
        for i, h in every:
            seq = list_ref[0, g * GROUP + i]
            found = jnp.where(
                lane < lengths[i], jnp.exp2((scores[i, h] - tops[i, h]) * scale2), 0.0
            )
            old = best[seq, h]
            new = jnp.maximum(old, tops[i, h])
            best[seq, h] = new
            keeps[i, h] = jnp.exp2((old - new) * scale2)
            adds[i, h] = jnp.exp2((tops[i, h] - new) * scale2)
            weight[seq, h] = weight[seq, h] * keeps[i, h] + found * adds[i, h]
            weights[i, h] = found
        return weights, keeps, adds

    def take(g, i, pair, softened):
        weights, keeps, adds = softened
        seq, slot = list_ref[0, g * GROUP + i], list_ref[1, g * GROUP + i]
        w2 = jnp.concatenate([weights[i, 2 * pair], weights[i, 2 * pair + 1]], axis=0)
        v2 = jnp.concatenate([value_buf[slot, 2 * pair], value_buf[slot, 2 * pair + 1]], axis=1)
        found = _dot(w2.astype(jnp.bfloat16), v2, NN)
        for e in range(2):
            h = 2 * pair + e
            mine = found[e * group_rows : (e + 1) * group_rows, e * width : (e + 1) * width]
            total[seq, h] = total[seq, h] * keeps[i, h] + mine * adds[i, h]

    wait(-(early // GROUP))
    for i, pair in both:
        ask(0, i, pair)

    def step(fetch, g, carry):
        q = g + RING - 2 - held_groups
        if not fetch:
            pl.when(q >= RING)(lambda: start_rest(q))
        wait(g - early // GROUP)
        softened = soften(g - 1)
        for at in range(len(both) + LAG):
            if at >= LAG:
                take(g - 1, *both[at - LAG], softened)
            if at < len(both):
                ask(g, *both[at])
            if fetch and at % 2 and at // 2 < GROUP:
                issue(q, at // 2)
        return carry

    steady = jnp.minimum(held_groups + 2, groups)
    settled = jnp.maximum(full - RING + 2 + held_groups, steady)

    def phase(p, carry):
        lax.fori_loop(
            jnp.where(p == 0, 1, settled),
            jnp.where(p == 0, steady, groups),
            functools.partial(step, False),
            0,
        )
        lax.fori_loop(
            jnp.where(p == 0, steady, 0),
            jnp.where(p == 0, settled, 0),
            functools.partial(step, True),
            0,
        )
        return carry

    lax.fori_loop(0, 2, phase, 0)
    last = jnp.maximum(groups - 1, 0)
    softened = soften(last)
    for i, pair in both:
        take(last, i, pair, softened)

    columns = heads * per_block
    across = blocks // lines
    fit = 128 // (3 * columns)
    stat_lane = lax.broadcasted_iota(jnp.int32, (group_rows, width), 1)
    for a in range(across):
        stats = {}
        for floor in range(lines):
            b = floor * across + a
            tile, base = floor // fit, (floor % fit) * 3 * columns
            stat = stats.get(tile, jnp.zeros((group_rows, width), jnp.float32))
            coded = []
            for c in range(columns):
                h, s = c // per_block, b * per_block + c % per_block
                sums = total[s, h]
                mass = jnp.sum(weight[s, h], axis=1, keepdims=True)
                largest = jnp.maximum(jnp.max(jnp.abs(sums), axis=1, keepdims=True), TINY)
                coded.append(jnp.round(sums * (CODE / largest)))
                stat = jnp.where(stat_lane == base + c, best[s, h], stat)
                stat = jnp.where(
                    stat_lane == base + columns + c, jnp.broadcast_to(mass, stat.shape), stat
                )
                stat = jnp.where(
                    stat_lane == base + 2 * columns + c,
                    jnp.broadcast_to(largest * (1.0 / CODE), stat.shape),
                    stat,
                )
            stats[tile] = stat
            for c in range(0, columns, 2):
                code_ref[b, c * group_rows : (c + 2) * group_rows] = (
                    jnp.concatenate(coded[c : c + 2], axis=0)
                    .astype(jnp.int32)
                    .astype(code_ref.dtype)
                )
        for tile, stat in stats.items():
            stat_ref[a, tile] = stat


def fold(codes, stats, columns, group_rows, scale2):
    top = functools.reduce(jnp.maximum, stats)
    lanes = top.shape[1]
    mass = jnp.zeros_like(top)
    sizes = []
    for stat in stats:
        factor = jnp.exp2((stat - top) * scale2)
        mass = mass + stat * pltpu.roll(factor, columns, 1)
        sizes.append(factor * pltpu.roll(stat, lanes - 2 * columns, 1))
    return top, mass, sizes


def combine(codes, sizes, columns, group_rows):
    sums = [jnp.zeros_like(sizes[0]) for _ in range(columns)]
    for code, size in zip(codes, sizes):
        wide = code[...].astype(jnp.int32).astype(jnp.float32)
        for c in range(columns):
            sums[c] = sums[c] + wide[c * group_rows : (c + 1) * group_rows] * jnp.broadcast_to(
                size[:, c : c + 1], size.shape
            )
    return sums


def exchange_kernel(
    n,
    parts,
    heads,
    code_ref,
    stat_ref,
    q_ref,
    key_ref,
    value_ref,
    out_ref,
    near,
    near_stat,
    folded,
    folded_stat,
    far,
    far_stat,
    near_send,
    near_recv,
    stat_send,
    stat_recv,
    far_send,
    far_recv,
):
    me = lax.axis_index("kv")
    plane, lines = split(n)
    spot, line = lax.rem(me, plane), me // plane
    group_rows, width = stat_ref.shape[2:]
    columns = code_ref.shape[1] // group_rows
    per_block = columns // heads
    across = plane // parts
    fit = 128 // (3 * columns)
    scale2 = math.log2(math.e) / math.sqrt(width)
    spots = [lax.rem(spot + k, plane) for k in range(1, plane)]
    floors = nearest(line, lines)[::-1] + [line]
    arrived = greet([line * plane + p for p in spots] + [f * plane + spot for f in floors[:-1]])

    def stat_copy(p, other, source):
        return pltpu.make_async_remote_copy(
            src_ref=stat_ref.at[other // parts],
            dst_ref=near_stat.at[source],
            send_sem=stat_send.at[p],
            recv_sem=stat_recv.at[source],
            device_id={"kv": line * plane + other},
            device_id_type=MESH,
        )

    def near_copy(k, floor, p, other, source):
        return pltpu.make_async_remote_copy(
            src_ref=code_ref.at[floor * across + other // parts],
            dst_ref=near.at[floor, source],
            send_sem=near_send.at[k, p],
            recv_sem=near_recv.at[floor, source],
            device_id={"kv": line * plane + other},
            device_id_type=MESH,
        )

    def far_copies(k, floor, source):
        return [
            pltpu.make_async_remote_copy(
                src_ref=src.at[k],
                dst_ref=dst.at[source],
                send_sem=far_send.at[e, k],
                recv_sem=far_recv.at[e, source],
                device_id={"kv": floor * plane + spot},
                device_id_type=MESH,
            )
            for e, (src, dst) in enumerate(((folded_stat, far_stat), (folded, far)))
        ]

    arrived()
    copies = []

    def send(copy):
        copy.start()
        copies.append(copy)

    for p, other in enumerate(spots):
        send(stat_copy(p, other, spot))
    for k, floor in enumerate(floors):
        for p, other in enumerate(spots):
            send(near_copy(k, floor, p, other, spot))
    for p, other in enumerate(spots):
        stat_copy(p, other, other).wait_recv()

    def aligned(ref, index, floor):
        if fit >= lines:
            tile, at = ref[index, 0], floor
        else:
            tile, at = ref[index, floor // fit], lax.rem(floor, fit)
        return pltpu.roll(tile, lax.rem(width - at * 3 * columns, width), 1)

    stat_lane = lax.broadcasted_iota(jnp.int32, (group_rows, width), 1)
    own = None
    for k, floor in enumerate(floors):
        stats = [aligned(stat_ref, spot // parts, floor)]
        stats += [aligned(near_stat, other, floor) for other in spots]
        for p, other in enumerate(spots):
            near_copy(k, floor, p, other, other).wait_recv()
        codes = [code_ref.at[floor * across + spot // parts]]
        codes += [near.at[floor, other] for other in spots]
        top, mass, sizes = fold(codes, stats, columns, group_rows, scale2)
        if k == lines - 1:
            own = top, mass, combine(codes, sizes, columns, group_rows)
            break
        size = jnp.maximum(functools.reduce(jnp.add, sizes), TINY)
        inverse = 1.0 / size
        sums = combine(codes, [s * inverse for s in sizes], columns, group_rows)
        folded_stat[k] = jnp.where(
            stat_lane < columns,
            top,
            jnp.where(stat_lane < 2 * columns, mass, pltpu.roll(size, 2 * columns, 1)),
        )
        for c in range(0, columns, 2):
            folded[k, c * group_rows : (c + 2) * group_rows] = (
                jnp.round(jnp.concatenate(sums[c : c + 2], axis=0))
                .astype(jnp.int32)
                .astype(folded.dtype)
            )
        for copy in far_copies(k, floor, line):
            send(copy)
    for k, floor in enumerate(floors[:-1]):
        for copy in far_copies(k, floor, floor):
            copy.wait_recv()
    stats = [far_stat[floor] for floor in floors[:-1]]
    own_top, own_mass, own_sums = own
    top = functools.reduce(jnp.maximum, stats, own_top)
    own_factor = jnp.exp2((own_top - top) * scale2)
    mass = own_mass * pltpu.roll(own_factor, columns, 1)
    sums = [s * jnp.broadcast_to(own_factor[:, c : c + 1], s.shape) for c, s in enumerate(own_sums)]
    sizes = []
    for stat in stats:
        factor = jnp.exp2((stat - top) * scale2)
        mass = mass + stat * pltpu.roll(factor, columns, 1)
        sizes.append(factor * pltpu.roll(stat, width - 2 * columns, 1))
    more = combine([far.at[floor] for floor in floors[:-1]], sizes, columns, group_rows)
    sums = [a + b for a, b in zip(sums, more)]
    for h in range(heads):
        wide = q_ref[h].astype(jnp.float32)
        results = []
        for j in range(per_block):
            c = h * per_block + j
            s = (me // parts) * per_block + j
            rows = slice(j * group_rows, (j + 1) * group_rows) if parts == 1 else slice(None)
            query = wide[rows]
            shape = query.shape
            fresh_key = jnp.broadcast_to(key_ref[s][h : h + 1].astype(jnp.float32), shape)
            fresh_value = jnp.broadcast_to(value_ref[s][h : h + 1].astype(jnp.float32), shape)
            new = jnp.broadcast_to(jnp.sum(query * fresh_key, axis=1, keepdims=True), shape)

            def mine(x):
                if parts == 1:
                    return x
                size = group_rows // parts
                picked = x[:size]
                for p in range(1, parts):
                    picked = jnp.where(
                        lax.rem(me, parts) == p, x[p * size : (p + 1) * size], picked
                    )
                return picked

            old = mine(jnp.broadcast_to(top[:, c : c + 1], top.shape))
            old_mass = mine(jnp.broadcast_to(mass[:, columns + c : columns + c + 1], top.shape))
            old_sum = mine(sums[c])
            highest = jnp.maximum(old, new)
            old_part = jnp.exp2((old - highest) * scale2)
            new_part = jnp.exp2((new - highest) * scale2)
            results.append(
                (old_sum * old_part + new_part * fresh_value) / (old_mass * old_part + new_part)
            )
        out_ref[h] = jnp.concatenate(results, axis=0).astype(out_ref.dtype)
    for copy in copies:
        copy.wait_send()


def far_off(x):
    return pltpu.with_memory_space_constraint(x, pltpu.HBM)


def on_device(n, queries, key_cache, value_cache, key_new, value_new, lengths, page_table):
    heads, local_rows, width = queries.shape
    seqs = lengths.shape[0]
    slots = page_table.shape[0] // seqs
    pages_here, _, page_len, _ = key_cache.shape
    group_rows = local_rows * n // seqs
    parts = max(1, group_rows // local_rows)
    blocks = n // parts
    columns = heads * (seqs // blocks)
    plane, lines = split(n)
    listed = -(-(pages_here + GROUP) // 128) * 128
    fetched = pages_here // 4
    spare = GROUP * RING
    held = fetched + spare
    tiles = -(-lines // (128 // (3 * columns)))
    vmem = pl.BlockSpec(memory_space=VMEM)
    smem = pl.BlockSpec(memory_space=pltpu.SMEM)
    hbm = pl.BlockSpec(memory_space=pltpu.HBM)
    sends = (lines - 1) + (plane - 1) * lines

    every_query, pages, key_buf, value_buf = pl.pallas_call(
        functools.partial(gather_kernel, n, pages_here, page_len, fetched, spare),
        out_shape=(
            jax.ShapeDtypeStruct((n,) + queries.shape, queries.dtype),
            jax.ShapeDtypeStruct((8, listed), jnp.int32),
            VMEM((held,) + key_cache.shape[1:], key_cache.dtype),
            VMEM((held,) + value_cache.shape[1:], value_cache.dtype),
        ),
        in_specs=[hbm] * 5,
        out_specs=(vmem, vmem, vmem, vmem),
        scratch_shapes=[
            VMEM((seqs, slots), jnp.int32),
            pltpu.SMEM((seqs,), jnp.int32),
            pltpu.SemaphoreType.DMA((sends,)),
            pltpu.SemaphoreType.DMA((n,)),
            pltpu.SemaphoreType.DMA((3,)),
            pltpu.SemaphoreType.DMA((2, CHUNKS)),
        ],
        compiler_params=pltpu.CompilerParams(
            collective_id=0, has_side_effects=True, vmem_limit_bytes=6 * 1024 * 1024
        ),
        name="gather_queries",
    )(far_off(queries), far_off(page_table.reshape(seqs, slots)), far_off(lengths), key_cache, value_cache)

    codes, stats, _, _ = pl.pallas_call(
        functools.partial(attend_kernel, group_rows, blocks, lines),
        out_shape=(
            jax.ShapeDtypeStruct((blocks, columns * group_rows, width), jnp.int16),
            jax.ShapeDtypeStruct((plane // parts, tiles, group_rows, width), jnp.float32),
            VMEM(key_buf.shape, key_buf.dtype),
            VMEM(value_buf.shape, value_buf.dtype),
        ),
        in_specs=[smem, vmem, hbm, hbm, vmem, vmem],
        out_specs=(vmem, vmem, vmem, vmem),
        input_output_aliases={4: 2, 5: 3},
        scratch_shapes=[
            VMEM((seqs, heads // 2, 2 * group_rows, width), queries.dtype),
            VMEM((GROUP, heads, group_rows, page_len), jnp.float32),
            VMEM((seqs, heads, group_rows, page_len), jnp.float32),
            VMEM((seqs, heads, group_rows, page_len), jnp.float32),
            VMEM((seqs, heads, group_rows, width), jnp.float32),
            pltpu.SemaphoreType.DMA((RING,)),
            pltpu.SemaphoreType.DMA((RING,)),
        ],
        compiler_params=pltpu.CompilerParams(vmem_limit_bytes=10 * 1024 * 1024),
        name="attend_pages",
    )(pages, every_query, key_cache, value_cache, key_buf, value_buf)

    code = (columns * group_rows, width)
    stat = (group_rows, width)
    return pl.pallas_call(
        functools.partial(exchange_kernel, n, parts, heads),
        out_shape=jax.ShapeDtypeStruct(queries.shape, jnp.bfloat16),
        in_specs=[vmem] * 5,
        out_specs=vmem,
        scratch_shapes=[
            VMEM((lines, plane) + code, jnp.int16),
            VMEM((plane, tiles) + stat, jnp.float32),
            VMEM((lines,) + code, jnp.int16),
            VMEM((lines,) + stat, jnp.float32),
            VMEM((lines,) + code, jnp.int16),
            VMEM((lines,) + stat, jnp.float32),
            pltpu.SemaphoreType.DMA((lines, plane)),
            pltpu.SemaphoreType.DMA((lines, plane)),
            pltpu.SemaphoreType.DMA((plane,)),
            pltpu.SemaphoreType.DMA((plane,)),
            pltpu.SemaphoreType.DMA((2, lines)),
            pltpu.SemaphoreType.DMA((2, lines)),
        ],
        compiler_params=pltpu.CompilerParams(
            collective_id=1, has_side_effects=True, vmem_limit_bytes=16 * 1024 * 1024
        ),
        name="exchange_and_finish",
    )(codes, stats, queries, key_new, value_new)


def solution(mesh):
    placed = (
        P("head", "kv", None),
        P("kv", "head", None, None),
        P("kv", "head", None, None),
        P(None, "head", None),
        P(None, "head", None),
        P(),
        P(),
    )
    return jax.shard_map(
        functools.partial(on_device, mesh.shape["kv"]),
        mesh=mesh,
        in_specs=placed,
        out_specs=P("head", "kv", None),
        check_vma=False,
    )
```
